32 devices in a mesh: shard: 8 (over z, y), tp: 4 (over x, core).
Axes of the slice: x: 2, y: 2, z: 4, core: 2. Of those that a mesh axis runs over, the one named last changes fastest.
Arguments:
- weight_query: bfloat16 [12288, 12288], P('shard', 'tp'), may hold values from -0.078125 to 0.078125
- low_query: bfloat16 [12288, 64], P('shard'), may hold values from -0.0546875 to 0.0546875
- high_query: bfloat16 [64, 12288], P(None, 'tp'), may hold values from -0.75 to 0.75
- weight_key: bfloat16 [12288, 12288], P('shard', 'tp'), may hold values from -0.078125 to 0.078125
- low_key: bfloat16 [12288, 64], P('shard'), may hold values from -0.0546875 to 0.0546875
- high_key: bfloat16 [64, 12288], P(None, 'tp'), may hold values from -0.75 to 0.75
- weight_value: bfloat16 [12288, 12288], P('shard', 'tp'), may hold values from -0.078125 to 0.078125
- low_value: bfloat16 [12288, 64], P('shard'), may hold values from -0.0546875 to 0.0546875
- high_value: bfloat16 [64, 12288], P(None, 'tp'), may hold values from -0.75 to 0.75
- norm_train: float32 [12288], P(('shard', 'tp')), may hold values from 0.25 to 1.75
- norm_step: float32 [12288], P(('shard', 'tp')), may hold values from -0.3 to 0.3
Outputs:
- ready_query: bfloat16 [12288, 12288], P(None, ('tp', 'shard'))
- ready_key: bfloat16 [12288, 12288], P(None, ('tp', 'shard'))
- ready_value: bfloat16 [12288, 12288], P(None, ('tp', 'shard'))
- column_query: float32 [12288], P(('tp', 'shard'))
- column_key: float32 [12288], P(('tp', 'shard'))
- column_value: float32 [12288], P(('tp', 'shard'))
- serve_norm: bfloat16 [12288], replicated
The draws below stay inside these ranges and needn't reach their ends.
All inputs are finite; a program needn't handle non-finite values. Where the reference program divides by a largest or mean magnitude, that divisor is 1e-20 or more.
Results may differ from the reference program's by a relative error of at most 0.001.
Values may be sent and summed in bfloat16 or wider, within the bound.
No kernel may reach another device: no remote copies, remote signals or barrier semaphores. Data moves between devices by JAX's collectives and lax.ppermute only.
A program may use at most 192 MiB of HBM per device.

```python
import jax
import jax.numpy as jnp

D_MODEL = 12288
Q_DIM = 12288
KV_DIM = 12288
RANK = 64


def with_spikes(values, key, source, target, parts, factor):
    owner, partner = [(jnp.arange(values.shape[position]) // (values.shape[position] // parts)).reshape([-1 if axis == position else 1 for axis in range(values.ndim)]) for position in (source, target)]
    chosen = jax.random.permutation(key, parts)[partner]
    strong = (owner == chosen) | (owner == (partner + parts // 2) % parts)
    return jnp.where(strong, factor * values, values)


def levels(stream_key, dims, shards, smallest, largest):
    loudness = 1.0
    for dim, parts in shards:
        draws = jax.random.uniform(jax.random.fold_in(jax.random.fold_in(stream_key, 6), dim), (parts,), jnp.float32, smallest / len(shards), largest / len(shards))
        loudness = loudness * jnp.repeat(jnp.exp(draws), dims[dim] // parts).reshape((-1,) + (1,) * (len(dims) - 1 - dim))
    return loudness


def bell_draw(key, extent, spread, bound, cuts=(), kind=jnp.bfloat16):
    loudness = levels(key, extent, cuts, -0.22, 0.18) if cuts else 1.0
    values = jax.random.normal(key, extent, jnp.float32) * spread * loudness
    return jnp.minimum(jnp.maximum(values, -bound), bound).astype(kind)


def heavy_noise(key, extent, width, most, shards, heavy, kind=jnp.bfloat16):
    array = width * jax.random.normal(key, extent, jnp.float32)
    if shards:
        array = array * levels(key, extent, shards, -0.22, 0.18)
    return jnp.clip(with_spikes(array, jax.random.fold_in(key, 3), *heavy), -most, most).astype(kind)


def setup_inputs(seed: int = 0) -> dict:
    seeds = jax.random.split(jax.random.key(seed), 12)
    return {
        "weight_query": heavy_noise(seeds[0], (D_MODEL, Q_DIM), D_MODEL ** -0.5, 0.078125, ((0, 8), (1, 4)), (0, 1, 8, 2.0)),
        "low_query": bell_draw(seeds[1], (D_MODEL, RANK), D_MODEL ** -0.5, 0.0546875, ((0, 8),)),
        "high_query": bell_draw(seeds[2], (RANK, Q_DIM), RANK ** -0.5, 0.75, ((1, 4),)),
        "weight_key": heavy_noise(seeds[3], (D_MODEL, KV_DIM), D_MODEL ** -0.5, 0.078125, ((0, 8), (1, 4)), (0, 1, 8, 2.0)),
        "low_key": bell_draw(seeds[4], (D_MODEL, RANK), D_MODEL ** -0.5, 0.0546875, ((0, 8),)),
        "high_key": bell_draw(seeds[5], (RANK, KV_DIM), RANK ** -0.5, 0.75, ((1, 4),)),
        "weight_value": heavy_noise(seeds[6], (D_MODEL, KV_DIM), D_MODEL ** -0.5, 0.078125, ((0, 8), (1, 4)), (0, 1, 8, 2.0)),
        "low_value": bell_draw(seeds[7], (D_MODEL, RANK), D_MODEL ** -0.5, 0.0546875, ((0, 8),)),
        "high_value": bell_draw(seeds[8], (RANK, KV_DIM), RANK ** -0.5, 0.75, ((1, 4),)),
        "norm_train": jnp.clip(1.0 + 0.15 * jax.random.normal(seeds[9], (D_MODEL,), jnp.float32), 0.25, 1.75),
        "norm_step": jnp.clip(jax.random.uniform(seeds[10], (D_MODEL,), jnp.float32, -0.3, 0.3) * levels(seeds[10], (D_MODEL,), ((0, 32),), -0.4, 0.0), -0.3, 0.3),
    }


mix_rate = 0.5


def reference(weight_query, low_query, high_query, weight_key, low_key, high_key, weight_value, low_value, high_value, norm_train, norm_step):
    latest_query = weight_query.astype(jnp.float32) + mix_rate * jnp.dot(low_query, high_query, preferred_element_type=jnp.float32)
    latest_key = weight_key.astype(jnp.float32) + mix_rate * jnp.dot(low_key, high_key, preferred_element_type=jnp.float32)
    latest_value = weight_value.astype(jnp.float32) + mix_rate * jnp.dot(low_value, high_value, preferred_element_type=jnp.float32)
    column_query = jnp.sum(jnp.abs(latest_query), axis=0) / D_MODEL
    ready_query = (latest_query / column_query).astype(jnp.bfloat16)
    column_key = jnp.sum(jnp.abs(latest_key), axis=0) / D_MODEL
    ready_key = (latest_key / column_key).astype(jnp.bfloat16)
    column_value = jnp.sum(jnp.abs(latest_value), axis=0) / D_MODEL
    ready_value = (latest_value / column_value).astype(jnp.bfloat16)
    serve_norm = (norm_train + norm_step).astype(jnp.bfloat16)
    return ready_query, ready_key, ready_value, column_query, column_key, column_value, serve_norm
```

```python
import jax
import jax.numpy as jnp
from jax import lax
from jax.experimental import pallas as pl
from jax.experimental.pallas import tpu as pltpu
from jax.sharding import PartitionSpec as P

mix_rate = 0.5


def merged(weight, low_t, high):
    product = lax.dot_general(
        low_t, high, (((0,), (0,)), ((), ())), preferred_element_type=jnp.float32
    )
    return weight.astype(jnp.float32) + mix_rate * product


def stats_kernel(weight, low_t, high, out):
    latest = merged(weight[...], low_t[...], high[...])
    out[...] = jnp.sum(jnp.abs(latest), axis=0, keepdims=True)


def stats(weight, low_t, high):
    rows, columns = weight.shape
    rank = high.shape[0]
    block = 512 if columns % 512 == 0 else 128
    return pl.pallas_call(
        stats_kernel,
        grid=(columns // block,),
        in_specs=[
            pl.BlockSpec((rows, block), lambda i: (0, i)),
            pl.BlockSpec((rank, rows), lambda i: (0, 0)),
            pl.BlockSpec((rank, block), lambda i: (0, i)),
        ],
        out_specs=pl.BlockSpec((1, block), lambda i: (0, i)),
        out_shape=jax.ShapeDtypeStruct((1, columns), jnp.float32),
        cost_estimate=pl.CostEstimate(
            flops=2 * rows * columns * rank, bytes_accessed=2 * rows * columns, transcendentals=0
        ),
        name="stats",
    )(weight, low_t, high)


def scale_kernel(where, weight, low_t, high, scale, out):
    latest = merged(weight[...], low_t[...], high[...])
    out[...] = (latest * scale[...]).astype(jnp.bfloat16)


def scaled(where, weight, low_t, high, scale, parts, whole):
    rows, columns = weight.shape
    rank = high.shape[0]
    width = columns // parts
    block = rows // 4 if rows % 512 == 0 else rows
    steps = rows // block
    out_map = (lambda i, d: (d[0] * steps + i, 0)) if whole else (lambda i, d: (i, 0))
    return pl.pallas_call(
        scale_kernel,
        grid_spec=pltpu.PrefetchScalarGridSpec(
            num_scalar_prefetch=1,
            grid=(steps,),
            in_specs=[
                pl.BlockSpec((block, width), lambda i, d: (i, d[0])),
                pl.BlockSpec((rank, block), lambda i, d: (0, i)),
                pl.BlockSpec((rank, width), lambda i, d: (0, d[0])),
                pl.BlockSpec((1, width), lambda i, d: (0, d[0])),
            ],
            out_specs=pl.BlockSpec((block, width), out_map),
        ),
        out_shape=jax.ShapeDtypeStruct((rows * parts if whole else rows, width), jnp.bfloat16),
        cost_estimate=pl.CostEstimate(
            flops=2 * rows * width * rank, bytes_accessed=4 * rows * width, transcendentals=0
        ),
        name="scaled",
    )(where, weight, low_t, high, scale)


def put_kernel(where, source, whole, out):
    out[...] = source[...]


def put(where, source, whole):
    rows, width = source.shape
    block = rows // 4 if rows % 512 == 0 else rows
    steps = rows // block
    return pl.pallas_call(
        put_kernel,
        grid_spec=pltpu.PrefetchScalarGridSpec(
            num_scalar_prefetch=1,
            grid=(steps,),
            in_specs=[
                pl.BlockSpec((block, width), lambda i, d: (i, 0)),
                pl.BlockSpec(memory_space=pl.ANY),
            ],
            out_specs=pl.BlockSpec((block, width), lambda i, d: (d[0] * steps + i, 0)),
        ),
        out_shape=jax.ShapeDtypeStruct(whole.shape, whole.dtype),
        input_output_aliases={2: 0},
        cost_estimate=pl.CostEstimate(
            flops=rows * width, bytes_accessed=4 * rows * width, transcendentals=0
        ),
        name="put",
    )(where, source, whole)


def exchanged(piece, axis, members):
    spread = jnp.broadcast_to(piece, (members, piece.shape[1]))
    return lax.all_to_all(spread, axis, split_axis=0, concat_axis=0, tiled=True)


def order(shards):
    half = shards // 2
    far, near = list(range(half, shards))[::-1], list(range(1, half))
    mixed = []
    while far or near:
        mixed += [far.pop(0)] if far else []
        mixed += [near.pop(0)] if near else []
    return mixed


def fast_body(shards, cuts, *args):
    weights, lows, highs = args[0:9:3], args[1:9:3], args[2:9:3]
    lows = [low.T for low in lows]
    columns = weights[0].shape[1]
    width = columns // shards
    d_model = weights[0].shape[0] * shards
    norm = (args[9] + args[10]).astype(jnp.bfloat16)
    norm = exchanged(norm[None], "tp", cuts).reshape(1, -1).astype(jnp.float32)
    parts = [stats(w, l, h) for w, l, h in zip(weights, lows, highs)]
    whole = exchanged(jnp.concatenate(parts + [norm], axis=1), "shard", shards)
    total = jnp.sum(whole[:, : 3 * columns], axis=0, keepdims=True)
    serve_norm = whole[:, 3 * columns :].astype(jnp.bfloat16).reshape(-1)
    scales = jnp.split(total / d_model, 3, axis=1)
    place = lax.axis_index("shard")
    ready = []
    for w, l, h, scale in zip(weights, lows, highs, scales):
        inverse = 1.0 / scale
        arrived = []
        for r in order(shards):
            where = (place ^ r).reshape(1)
            block = scaled(where, w, l, h, inverse, shards, False)
            pairs = [(i, i ^ r) for i in range(shards)]
            arrived.append((where, lax.ppermute(block, "shard", pairs)))
        out = scaled(place.reshape(1), w, l, h, inverse, shards, True)
        for where, block in arrived:
            out = put(where, block, out)
        ready.append(out)
    own = [lax.dynamic_slice_in_dim(c[0], place * width, width) for c in scales]
    return (*ready, *own, serve_norm)


def plain_body(shards, *args):
    d_model = args[0].shape[0] * shards
    latest = [
        w.astype(jnp.float32) + mix_rate * jnp.dot(l, h, preferred_element_type=jnp.float32)
        for w, l, h in zip(args[0:9:3], args[1:9:3], args[2:9:3])
    ]
    totals = lax.psum(tuple(jnp.sum(jnp.abs(x), axis=0) for x in latest), "shard")
    columns = [t / d_model for t in totals]
    ready = [
        lax.all_to_all(
            (x / c).astype(jnp.bfloat16), "shard", split_axis=1, concat_axis=0, tiled=True
        )
        for x, c in zip(latest, columns)
    ]
    place = lax.axis_index("shard")
    width = ready[0].shape[1]
    own = [lax.dynamic_slice_in_dim(c, place * width, width) for c in columns]
    serve_norm = lax.all_gather(
        (args[9] + args[10]).astype(jnp.bfloat16), ("shard", "tp"), axis=0, tiled=True
    )
    return (*ready, *own, serve_norm)


def solution(mesh):
    shards, cuts = mesh.shape["shard"], mesh.shape["tp"]
    one = (P("shard", "tp"), P("shard", None), P(None, "tp"))
    norm = P(("shard", "tp"))
    across = P(None, ("tp", "shard"))

    def body(*args):
        rows, columns = args[0].shape
        if (columns // shards) % 128 == 0 and rows % 128 == 0 and shards & (shards - 1) == 0:
            return fast_body(shards, cuts, *args)
        return plain_body(shards, *args)

    return jax.shard_map(
        body,
        mesh=mesh,
        in_specs=one * 3 + (norm, norm),
        out_specs=(across,) * 3 + (P(("tp", "shard")),) * 3 + (P(),),
        check_vma=False,
    )
```

```python
import jax
import jax.numpy as jnp
from jax import lax
from jax.experimental import pallas as pl
from jax.experimental.pallas import tpu as pltpu
from jax.sharding import PartitionSpec as P


mix_rate = 0.5


def merged(weight, low_t, high):
    product = lax.dot_general(
        low_t, high, (((0,), (0,)), ((), ())), preferred_element_type=jnp.float32
    )
    return weight.astype(jnp.float32) + mix_rate * product


def stats_kernel(weight, low_t, high, out):
    latest = merged(weight[...], low_t[...], high[...])
    out[...] = jnp.sum(jnp.abs(latest), axis=0, keepdims=True)


def stats(weight, low_t, high):
    rows, columns = weight.shape
    rank = high.shape[0]
    block = 512 if columns % 512 == 0 else 128
    return pl.pallas_call(
        stats_kernel,
        grid=(columns // block,),
        in_specs=[
            pl.BlockSpec((rows, block), lambda i: (0, i)),
            pl.BlockSpec((rank, rows), lambda i: (0, 0)),
            pl.BlockSpec((rank, block), lambda i: (0, i)),
        ],
        out_specs=pl.BlockSpec((1, block), lambda i: (0, i)),
        out_shape=jax.ShapeDtypeStruct((1, columns), jnp.float32),
        cost_estimate=pl.CostEstimate(
            flops=2 * rows * columns * rank, bytes_accessed=2 * rows * columns, transcendentals=0
        ),
        name="stats",
    )(weight, low_t, high)


def scale_kernel(where, weight, low_t, high, scale, out):
    latest = merged(weight[...], low_t[...], high[...])
    out[...] = (latest * scale[...]).astype(jnp.bfloat16)


def scaled(where, weight, low_t, high, scale, parts, whole):
    rows, columns = weight.shape
    rank = high.shape[0]
    width = columns // parts
    block = rows // 4 if rows % 512 == 0 else rows
    steps = rows // block
    out_map = (lambda i, d: (d[0] * steps + i, 0)) if whole else (lambda i, d: (i, 0))
    return pl.pallas_call(
        scale_kernel,
        grid_spec=pltpu.PrefetchScalarGridSpec(
            num_scalar_prefetch=1,
            grid=(steps,),
            in_specs=[
                pl.BlockSpec((block, width), lambda i, d: (i, d[0])),
                pl.BlockSpec((rank, block), lambda i, d: (0, i)),
                pl.BlockSpec((rank, width), lambda i, d: (0, d[0])),
                pl.BlockSpec((1, width), lambda i, d: (0, d[0])),
            ],
            out_specs=pl.BlockSpec((block, width), out_map),
        ),
        out_shape=jax.ShapeDtypeStruct((rows * parts if whole else rows, width), jnp.bfloat16),
        cost_estimate=pl.CostEstimate(
            flops=2 * rows * width * rank, bytes_accessed=4 * rows * width, transcendentals=0
        ),
        name="scaled",
    )(where, weight, low_t, high, scale)


def put_kernel(where, source, whole, out):
    out[...] = source[...]


def put(where, source, whole):
    rows, width = source.shape
    block = rows // 4 if rows % 512 == 0 else rows
    steps = rows // block
    return pl.pallas_call(
        put_kernel,
        grid_spec=pltpu.PrefetchScalarGridSpec(
            num_scalar_prefetch=1,
            grid=(steps,),
            in_specs=[
                pl.BlockSpec((block, width), lambda i, d: (i, 0)),
                pl.BlockSpec(memory_space=pl.ANY),
            ],
            out_specs=pl.BlockSpec((block, width), lambda i, d: (d[0] * steps + i, 0)),
        ),
        out_shape=jax.ShapeDtypeStruct(whole.shape, whole.dtype),
        input_output_aliases={2: 0},
        cost_estimate=pl.CostEstimate(
            flops=rows * width, bytes_accessed=4 * rows * width, transcendentals=0
        ),
        name="put",
    )(where, source, whole)


def exchanged(piece, axis, members):
    spread = jnp.broadcast_to(piece, (members, piece.shape[1]))
    return lax.all_to_all(spread, axis, split_axis=0, concat_axis=0, tiled=True)


def order(shards):
    half = shards // 2
    far, near = list(range(half, shards))[::-1], list(range(1, half))
    mixed = []
    while far or near:
        mixed += [far.pop(0)] if far else []
        mixed += [near.pop(0)] if near else []
    return mixed


def fast_body(shards, cuts, *args):
    weights, lows, highs = args[0:9:3], args[1:9:3], args[2:9:3]
    lows = [low.T for low in lows]
    columns = weights[0].shape[1]
    width = columns // shards
    d_model = weights[0].shape[0] * shards
    place = lax.axis_index("shard")
    norm = (args[9] + args[10]).astype(jnp.bfloat16).astype(jnp.float32)[None]
    parts = []
    for name, w, l, h in zip("qkv", weights, lows, highs):
        parts.append(stats(w, l, h))
    first = exchanged(parts[0], "shard", shards)
    later = exchanged(jnp.concatenate(parts[1:] + [norm], axis=1), "shard", shards)
    totals = [jnp.sum(first, axis=0, keepdims=True)]
    totals += jnp.split(jnp.sum(later[:, : 2 * columns], axis=0, keepdims=True), 2, axis=1)
    scales = [total / d_model for total in totals]
    ready = []
    for name, w, l, h, scale in zip("qkv", weights, lows, highs, scales):
        inverse = 1.0 / scale
        arrived = []
        for r in order(shards):
            where = (place ^ r).reshape(1)
            block = scaled(where, w, l, h, inverse, shards, False)
            pairs = [(i, i ^ r) for i in range(shards)]
            arrived.append((where, lax.ppermute(block, "shard", pairs)))
        if name == "k":
            mine = later[:, 2 * columns :].astype(jnp.bfloat16).reshape(1, -1)
            mine, block = lax.optimization_barrier((mine, arrived[0][1]))
            arrived[0] = (arrived[0][0], block)
            whole = exchanged(mine, "tp", cuts)
            whole = whole.reshape(cuts, shards, -1).transpose(1, 0, 2)
            serve_norm = whole.reshape(-1)
        out = scaled(place.reshape(1), w, l, h, inverse, shards, True)
        for where, block in arrived:
            out = put(where, block, out)
        ready.append(out)
    own = [lax.dynamic_slice_in_dim(c[0], place * width, width) for c in scales]
    return (*ready, *own, serve_norm)


def plain_body(shards, *args):
    d_model = args[0].shape[0] * shards
    latest = [
        w.astype(jnp.float32) + mix_rate * jnp.dot(l, h, preferred_element_type=jnp.float32)
        for w, l, h in zip(args[0:9:3], args[1:9:3], args[2:9:3])
    ]
    totals = lax.psum(tuple(jnp.sum(jnp.abs(x), axis=0) for x in latest), "shard")
    columns = [t / d_model for t in totals]
    ready = [
        lax.all_to_all(
            (x / c).astype(jnp.bfloat16), "shard", split_axis=1, concat_axis=0, tiled=True
        )
        for x, c in zip(latest, columns)
    ]
    place = lax.axis_index("shard")
    width = ready[0].shape[1]
    own = [lax.dynamic_slice_in_dim(c, place * width, width) for c in columns]
    serve_norm = lax.all_gather(
        (args[9] + args[10]).astype(jnp.bfloat16), ("shard", "tp"), axis=0, tiled=True
    )
    return (*ready, *own, serve_norm)


def solution(mesh):
    shards, cuts = mesh.shape["shard"], mesh.shape["tp"]
    one = (P("shard", "tp"), P("shard", None), P(None, "tp"))
    norm = P(("shard", "tp"))
    across = P(None, ("tp", "shard"))

    def body(*args):
        rows, columns = args[0].shape
        if (columns // shards) % 128 == 0 and rows % 128 == 0 and shards & (shards - 1) == 0:
            return fast_body(shards, cuts, *args)
        return plain_body(shards, *args)

    return jax.shard_map(
        body,
        mesh=mesh,
        in_specs=one * 3 + (norm, norm),
        out_specs=(across,) * 3 + (P(("tp", "shard")),) * 3 + (P(),),
        check_vma=False,
    )
```
